32 devices in a mesh: seq: 8 (over y, x, core), head: 4 (over z).
Axes of the slice: x: 2, y: 2, z: 4, core: 2. Of those that a mesh axis runs over, the one named last changes fastest.
Arguments:
- queries: bfloat16 [1024, 1024], P('seq', 'head'), may hold values from -24 to 24
- keys_values: bfloat16 [2, 1024, 128], P(None, 'seq'), may hold values from -6 to 6
- out_weight: bfloat16 [2560, 8, 128], P('head'), may hold values from -0.125 to 0.125
- out_grad: bfloat16 [1024, 2560], P('seq'), may hold values from -6 to 6
- positions: int32 [1024], replicated, may hold values from 0 to 1023, as said below
Outputs:
- d_query: bfloat16 [1024, 1024], P('seq', 'head')
- d_out_weight: float32 [2560, 8, 128], P('seq', 'head')
The draws below stay inside these ranges and needn't reach their ends.
Inputs may be any that keep to these rules, and one draw needn't show every extreme that they name: positions holds each of 0 to 1023 once, in runs of 64 consecutive rows with consecutive positions, each run starting at a row and a position that are multiples of 64.
All inputs are finite; a program needn't handle non-finite values.
Results may differ from the reference program's by a relative error of at most 0.007.
Values may be sent and summed in bfloat16 or wider, within the bound.
A program may use at most 64 MiB of HBM per device.

```python
import jax
import jax.numpy as jnp
from jax import lax

HD = 128
GROUP = 8
DW = 2560
TOK_DEV = 128
HQ = 8
KVH = 1
SEQ = 1024


def raw_pairs(key):
    base = jax.random.fold_in(key, 11)
    raw = jnp.clip(jax.random.normal(base, (2, SEQ, KVH * HD), jnp.float32), -6.0, 6.0)
    return raw


def draw_keys_values(key, part):
    raw = raw_pairs(key)
    return raw.astype(jnp.bfloat16)


def draw_queries(key, part):
    qkey = jax.random.fold_in(key, 23)
    base = jnp.clip(jax.random.normal(qkey, (SEQ, HQ, HD), jnp.float32), -6.0, 6.0)
    return base.reshape(SEQ, HQ * HD).astype(jnp.bfloat16)


def draw_positions(key, part):
    runs = 2 * SEQ // TOK_DEV
    half_run = TOK_DEV // 2
    order = jax.random.permutation(jax.random.fold_in(key, 41), runs).astype(jnp.int32)
    within = jnp.arange(half_run, dtype=jnp.int32)
    return (order[:, None] * half_run + within[None, :]).reshape(SEQ).astype(jnp.int32)


def with_spikes(array, key, source, target, shards_of, factor):
    owner, partner = [(jnp.arange(array.shape[position]) // (array.shape[position] // shards_of)).reshape([-1 if axis == position else 1 for axis in range(array.ndim)]) for position in (source, target)]
    chosen = jax.random.permutation(key, shards_of)[partner]
    strong = (owner == chosen) | (owner == (partner + shards_of // 2) % shards_of)
    return jnp.where(strong, factor * array, array)


def shard_levels(own_key, shape, cuts, least, top_value):
    loudness, own = 1.0, jax.random.fold_in(own_key, 6)
    for dim, blocks in cuts:
        heights = jnp.exp(jax.random.uniform(jax.random.fold_in(own, dim), (blocks,), jnp.float32, least / len(cuts), top_value / len(cuts)))
        loudness = loudness * jnp.repeat(heights, shape[dim] // blocks).reshape([-1 if axis == dim else 1 for axis in range(len(shape))])
    return loudness


def noise(key, dims, deviation, bound, pieces=(), kind=jnp.bfloat16):
    values = deviation * jax.random.normal(key, dims, jnp.float32)
    if pieces:
        values = values * shard_levels(key, dims, pieces, -0.22, 0.18)
    return jnp.clip(values, -bound, bound).astype(kind)


def bell_draw_with(key, dims, spread, most, cuts, heavy, kind=jnp.bfloat16):
    array = spread * jax.random.normal(key, dims, jnp.float32)
    if cuts:
        array = array * shard_levels(key, dims, cuts, -0.22, 0.18)
    return jnp.clip(with_spikes(array, jax.random.fold_in(key, 3), *heavy), -most, most).astype(kind)


def setup_inputs(seed: int = 0) -> dict:
    splits = jax.random.split(jax.random.key(seed), 6)
    return {
        "queries": draw_queries(jax.random.fold_in(splits[5], 71), 0),
        "keys_values": draw_keys_values(jax.random.fold_in(splits[5], 71), 0),
        "out_weight": noise(splits[2], (DW, HQ, HD), DW ** -0.5, 0.125, ((0, 4),)),
        "out_grad": bell_draw_with(splits[3], (SEQ, DW), 1.0, 6.0, ((0, 8),), (0, 1, 8, 2.0)),
        "positions": draw_positions(jax.random.fold_in(splits[5], 71), 0),
    }


big_negative = -1.0e30


def reference(queries, keys_values, out_weight, out_grad, positions):
    scale = HD ** -0.5
    d_attn = jnp.dot(out_grad, out_weight.reshape(DW, HQ * HD), preferred_element_type=jnp.float32).astype(jnp.bfloat16)
    query_heads = queries.reshape(SEQ, HQ, HD).transpose(1, 0, 2)
    grad_heads = d_attn.reshape(SEQ, HQ, HD).transpose(1, 0, 2)
    key_heads = jnp.repeat(keys_values[0].reshape(SEQ, KVH, HD).transpose(1, 0, 2), GROUP, axis=0)
    value_heads = jnp.repeat(keys_values[1].reshape(SEQ, KVH, HD).transpose(1, 0, 2), GROUP, axis=0)
    visible = positions[None, :] <= positions[:, None]

    def one_head(operands):
        query, key, value, grad = operands
        scores = jnp.dot(query, key.T, preferred_element_type=jnp.float32) * scale
        scores = jnp.where(visible, scores, big_negative)
        top = jnp.max(scores, axis=1, keepdims=True)
        weights = jnp.where(visible, jnp.exp(scores - top), 0.0)
        probs = weights / jnp.sum(weights, axis=1, keepdims=True)
        attn_full = jnp.dot(probs.astype(jnp.bfloat16), value, preferred_element_type=jnp.float32)
        delta = jnp.sum(grad.astype(jnp.float32) * attn_full, axis=1, keepdims=True)
        dprob = jnp.dot(grad, value.T, preferred_element_type=jnp.float32)
        dscore = (probs * (dprob - delta)).astype(jnp.bfloat16)
        dquery = jnp.dot(dscore, key, preferred_element_type=jnp.float32) * scale
        return attn_full.astype(jnp.bfloat16), dquery.astype(jnp.bfloat16)

    attn, d_query = lax.map(one_head, (query_heads, key_heads, value_heads, grad_heads))
    attn = attn.transpose(1, 0, 2).reshape(SEQ, HQ * HD)
    d_query = d_query.transpose(1, 0, 2).reshape(SEQ, HQ * HD)
    d_out_weight = lax.dot_general(out_grad, attn, (((0,), (0,)), ((), ())), preferred_element_type=jnp.float32)
    return d_query, d_out_weight.reshape(DW, HQ, HD)
```

```python
import functools

import jax
import jax.numpy as jnp
from jax import lax
from jax.experimental import pallas as pl
from jax.experimental.pallas import tpu as pltpu
from jax.sharding import PartitionSpec as P

HD = 128
GROUP = 8
RUN = 64
BIG_NEGATIVE = -1e30
MESH = pl.DeviceIdType.MESH


def remote(src, dst, send_sem, recv_sem, axis, peer):
    return pltpu.make_async_remote_copy(
        src_ref=src,
        dst_ref=dst,
        send_sem=send_sem,
        recv_sem=recv_sem,
        device_id={axis: peer},
        device_id_type=MESH,
    )


class Gather:
    def __init__(self, n, me, own, slots, send, relay, recv):
        self.n, self.me, self.own, self.slots = n, me, own, slots
        self.send, self.relay, self.recv = send, relay, recv
        self.core = lax.rem(me, 2)
        self.half = lax.div(me, 2)
        self.partner = me + 1 - 2 * self.core

    def peer(self, k):
        return 2 * lax.rem(self.half + k, self.n // 2) + self.core

    def copies(self):
        for k in range(self.n // 2):
            to = self.partner if k == 0 else self.peer(k)
            yield remote(
                self.own, self.slots.at[self.me], self.send.at[k], self.recv.at[self.me], "seq", to
            )

    def relay_copy(self, k):
        src = self.peer(k)
        return remote(
            self.slots.at[src],
            self.slots.at[src],
            self.relay.at[k],
            self.recv.at[src],
            "seq",
            self.partner,
        )

    def start(self):
        for copy in self.copies():
            copy.start()

    def arrived(self, src):
        remote(
            self.own, self.slots.at[src], self.send.at[0], self.recv.at[src], "seq", self.partner
        ).wait_recv()

    def pass_on(self, k):
        self.arrived(self.peer(k))
        self.relay_copy(k).start()

    def other(self, k):
        return self.peer(k) + 1 - 2 * self.core

    def finish(self):
        for copy in self.copies():
            copy.wait_send()
        for k in range(1, self.n // 2):
            self.relay_copy(k).wait_send()


def kernel(
    n,
    m,
    turn,
    pos_ref,
    q_ref,
    kv_ref,
    g_hbm,
    w_hbm,
    dq_ref,
    dw_ref,
    g_v,
    gt_v,
    w_v,
    kv_all,
    part,
    part_own,
    part_all,
    attn_own,
    attn_all,
    g_all,
    scores,
    local_sem,
    kv_send,
    kv_relay,
    kv_recv,
    at_send,
    at_relay,
    at_recv,
    g_send,
    g_recv,
    p_send,
    p_recv,
):
    me = lax.axis_index("seq")
    hme = lax.axis_index("head")
    tok = q_ref.shape[0]
    heads = q_ref.shape[1] // HD
    rows = g_all.shape[1]
    dz = w_v.shape[0]
    scale = HD ** (-0.5)

    g_copy = pltpu.make_async_copy(g_hbm, g_v, local_sem.at[0])
    w_copy = pltpu.make_async_copy(w_hbm, w_v, local_sem.at[1])
    g_copy.start()
    w_copy.start()

    barrier = pltpu.get_barrier_semaphore()
    for k in range(1, n):
        pl.semaphore_signal(
            barrier, inc=1, device_id={"seq": lax.rem(me + k, n)}, device_id_type=MESH
        )
    for k in range(1, m):
        pl.semaphore_signal(
            barrier, inc=1, device_id={"head": lax.rem(hme + k, m)}, device_id_type=MESH
        )
    pl.semaphore_wait(barrier, n + m - 2)

    group = lax.div(hme * heads, GROUP)
    columns = pl.ds(pl.multiple_of(group * HD, HD), HD)
    own_kv = kv_ref.at[:, :, columns]
    kv = Gather(n, me, own_kv, kv_all, kv_send, kv_relay, kv_recv)
    kv.start()
    kv_all[me] = own_kv[...]

    g_copy.wait()
    if turn:
        for j in range(n * rows // HD):
            gt_v[pl.ds(j * HD, HD), :] = g_v[:, pl.ds(j * HD, HD)].T

        def g_block(i):
            return gt_v.at[pl.ds(pl.multiple_of(i * rows, 16), rows)]

    else:

        def g_block(i):
            return g_v.at[i]

    def g_send_copy(k):
        to = lax.rem(me + k, n)
        return remote(g_block(to), g_all.at[me], g_send.at[k], g_recv.at[me], "seq", to)

    for k in range(1, n):
        g_send_copy(k).start()

    w_copy.wait()

    def partial(j):
        wide = heads * HD
        total = jnp.zeros((tok, wide), jnp.float32)
        if turn:
            lhs = g_v[:, pl.ds(pl.multiple_of(hme * dz, HD), dz)]
            for h in range(heads):
                piece = jnp.dot(
                    lhs, w_v[:, j * heads + h, :], preferred_element_type=jnp.float32
                )
                yield piece
        else:
            blocks = dz // rows
            for h in range(heads):
                total = jnp.zeros((tok, HD), jnp.float32)
                for b in range(blocks):
                    total = total + lax.dot_general(
                        g_v[hme * blocks + b],
                        w_v[pl.ds(b * rows, rows), j * heads + h, :],
                        (((0,), (0,)), ((), ())),
                        preferred_element_type=jnp.float32,
                    )
                yield total

    for j in range(m):
        for h, piece in enumerate(partial(j)):
            part[j, :, pl.ds(h * HD, HD)] = piece.astype(jnp.bfloat16)

    def p_copy(k):
        to = lax.rem(hme + k, m)
        return remote(part.at[to], part_all.at[hme], p_send.at[k], p_recv.at[hme], "head", to)

    for k in range(1, m):
        p_copy(k).start()

    for k in range(1, n // 2):
        kv.pass_on(k)
    for k in range(n // 2):
        kv.arrived(kv.other(k))

    query = jnp.concatenate([q_ref[:, pl.ds(h * HD, HD)] for h in range(heads)], axis=0)
    total_rows = heads * tok
    row = lax.broadcasted_iota(jnp.int32, (tok, 1), 0)
    lane = lax.broadcasted_iota(jnp.int32, (1, tok), 1)

    def run_positions(block, index):
        value = pos_ref[block * tok] + index
        for r in range(1, tok // RUN):
            start = pos_ref[block * tok + r * RUN] + index - r * RUN
            value = jnp.where(index >= r * RUN, start, value)
        return value

    own_pos = run_positions(me, row)
    query_pos = jnp.concatenate([own_pos] * heads, axis=0)
    step_blocks = min(n, 8)
    span = step_blocks * tok

    def keys(c, which):
        return kv_all[pl.ds(c * step_blocks, step_blocks), which].reshape(span, HD)

    def loop(body, init):
        if n == step_blocks:
            return body(0, init)
        return lax.fori_loop(0, n // step_blocks, body, init)

    def at(c):
        return pl.ds(c * span if isinstance(c, int) else pl.multiple_of(c * span, span), span)

    def score_step(c, top):
        value = lax.dot_general(
            query, keys(c, 0), (((1,), (1,)), ((), ())), preferred_element_type=jnp.float32
        )
        key_pos = jnp.concatenate(
            [run_positions(c * step_blocks + b, lane) for b in range(step_blocks)], axis=1
        )
        value = jnp.where(key_pos <= query_pos, value * scale, BIG_NEGATIVE)
        scores[:, at(c)] = value
        return jnp.maximum(top, jnp.max(value, axis=1, keepdims=True))

    top = loop(score_step, jnp.full((total_rows, 1), BIG_NEGATIVE, jnp.float32))

    def out_step(c, carry):
        norm, out = carry
        weights = jnp.exp(scores[:, at(c)] - top)
        scores[:, at(c)] = weights
        norm = norm + jnp.sum(weights, axis=1, keepdims=True)
        out = out + jnp.dot(
            weights.astype(jnp.bfloat16), keys(c, 1), preferred_element_type=jnp.float32
        )
        return norm, out

    norm, out = loop(
        out_step,
        (jnp.zeros((total_rows, 1), jnp.float32), jnp.zeros((total_rows, HD), jnp.float32)),
    )
    inverse = 1.0 / norm
    attn = out * inverse
    for h in range(heads):
        attn_own[:, pl.ds(h * HD, HD)] = attn[h * tok : (h + 1) * tok].astype(jnp.bfloat16)
    at_gather = Gather(n, me, attn_own, attn_all, at_send, at_relay, at_recv)
    at_gather.start()

    grad = part[hme].astype(jnp.float32)
    for k in range(1, m):
        src = lax.rem(hme + k, m)
        remote(
            part.at[0], part_all.at[src], p_send.at[k], p_recv.at[src], "head", src
        ).wait_recv()
        grad = grad + part_all[src].astype(jnp.float32)
    grad = jnp.concatenate(
        [grad[:, h * HD : (h + 1) * HD] for h in range(heads)], axis=0
    ).astype(jnp.bfloat16)
    delta = jnp.sum(grad.astype(jnp.float32) * attn, axis=1, keepdims=True)

    def grad_step(c, total):
        dprob = lax.dot_general(
            grad, keys(c, 1), (((1,), (1,)), ((), ())), preferred_element_type=jnp.float32
        )
        dscore = (scores[:, at(c)] * inverse * (dprob - delta)).astype(jnp.bfloat16)
        return total + jnp.dot(dscore, keys(c, 0), preferred_element_type=jnp.float32)

    d_rows = loop(grad_step, jnp.zeros((total_rows, HD), jnp.float32)) * scale
    for h in range(heads):
        dq_ref[:, pl.ds(h * HD, HD)] = d_rows[h * tok : (h + 1) * tok].astype(jnp.bfloat16)

    total = jnp.dot(g_block(me)[...], attn_own[...], preferred_element_type=jnp.float32)

    def g_arrived(src):
        remote(
            g_block(me), g_all.at[src], g_send.at[1], g_recv.at[src], "seq", src
        ).wait_recv()

    for k in range(1, n // 2):
        at_gather.pass_on(k)
    order = [at_gather.other(0)]
    for k in range(1, n // 2):
        order += [at_gather.peer(k), at_gather.other(k)]
    for index, src in enumerate(order):
        if index % 2 == 0:
            at_gather.arrived(src)
        g_arrived(src)
        total = total + jnp.dot(g_all[src], attn_all[src], preferred_element_type=jnp.float32)
    for h in range(heads):
        dw_ref[h] = total[:, h * HD : (h + 1) * HD]

    kv.finish()
    at_gather.finish()
    for k in range(1, n):
        g_send_copy(k).wait_send()
    for k in range(1, m):
        p_copy(k).wait_send()


def body(n, m, queries, keys_values, out_weight, out_grad, positions):
    tok, width = queries.shape
    heads = width // HD
    dz, all_heads, _ = out_weight.shape
    features = out_grad.shape[1]
    rows = features // n
    turn = rows % 16 == 0 and dz % HD == 0 and features % HD == 0
    bf16, f32 = jnp.bfloat16, jnp.float32
    if not turn:
        out_grad = out_grad.T.reshape(n, rows, tok)
    vmem = pl.BlockSpec(memory_space=pltpu.VMEM)
    anywhere = pl.BlockSpec(memory_space=pl.ANY)
    dma = pltpu.SemaphoreType.DMA
    d_query, d_weight = pl.pallas_call(
        functools.partial(kernel, n, m, turn),
        out_shape=(
            jax.ShapeDtypeStruct((tok, width), bf16),
            jax.ShapeDtypeStruct((heads, rows, HD), f32),
        ),
        in_specs=[
            pl.BlockSpec(memory_space=pltpu.SMEM),
            vmem,
            vmem,
            anywhere,
            anywhere,
        ],
        out_specs=(vmem, vmem),
        scratch_shapes=[
            pltpu.VMEM(out_grad.shape, bf16),
            pltpu.VMEM((features, tok) if turn else (16, HD), bf16),
            pltpu.VMEM(out_weight.shape, bf16),
            pltpu.VMEM((n, 2, tok, HD), bf16),
            pltpu.VMEM((m, tok, width), bf16),
            pltpu.VMEM((tok, width), f32),
            pltpu.VMEM((m, tok, width), bf16),
            pltpu.VMEM((tok, width), bf16),
            pltpu.VMEM((n, tok, width), bf16),
            pltpu.VMEM((n, rows, tok), bf16),
            pltpu.VMEM((heads * tok, n * tok), f32),
            dma((2,)),
            dma((n,)),
            dma((n,)),
            dma((n,)),
            dma((n,)),
            dma((n,)),
            dma((n,)),
            dma((n,)),
            dma((n,)),
            dma((m,)),
            dma((m,)),
        ],
        compiler_params=pltpu.CompilerParams(
            collective_id=0, has_side_effects=True, vmem_limit_bytes=56 * 1024 * 1024
        ),
    )(positions, queries, keys_values, out_grad, out_weight)
    return d_query, d_weight.transpose(1, 0, 2)


def solution(mesh):
    n, m = mesh.shape["seq"], mesh.shape["head"]
    return jax.shard_map(
        functools.partial(body, n, m),
        mesh=mesh,
        in_specs=(
            P("seq", "head"),
            P(None, "seq", None),
            P("head", None, None),
            P("seq", None),
            P(),
        ),
        out_specs=(P("seq", "head"), P("seq", "head", None)),
        check_vma=False,
    )
```

```python
import functools

import jax
import jax.numpy as jnp
from jax import lax
from jax.experimental import pallas as pl
from jax.experimental.pallas import tpu as pltpu
from jax.sharding import PartitionSpec as P

HD = 128
GROUP = 8
RUN = 64
VMEM_LIMIT = 67043328
BIG_NEGATIVE = -1e30
MESH = pl.DeviceIdType.MESH


def remote(src, dst, send_sem, recv_sem, axis, peer):
    return pltpu.make_async_remote_copy(
        src_ref=src,
        dst_ref=dst,
        send_sem=send_sem,
        recv_sem=recv_sem,
        device_id={axis: peer},
        device_id_type=MESH,
    )


class Gather:
    def __init__(self, n, me, own, slots, send, relay, recv):
        self.n, self.me, self.own, self.slots = n, me, own, slots
        self.send, self.relay, self.recv = send, relay, recv
        self.core = lax.rem(me, 2)
        self.half = lax.div(me, 2)
        self.partner = me + 1 - 2 * self.core

    def peer(self, k):
        return 2 * lax.rem(self.half + k, self.n // 2) + self.core

    def copies(self):
        for k in range(self.n // 2):
            to = self.partner if k == 0 else self.peer(k)
            yield remote(
                self.own, self.slots.at[self.me], self.send.at[k], self.recv.at[self.me], "seq", to
            )

    def relay_copy(self, k):
        src = self.peer(k)
        return remote(
            self.slots.at[src],
            self.slots.at[src],
            self.relay.at[k],
            self.recv.at[src],
            "seq",
            self.partner,
        )

    def start(self):
        for copy in self.copies():
            copy.start()

    def arrived(self, src):
        remote(
            self.own, self.slots.at[src], self.send.at[0], self.recv.at[src], "seq", self.partner
        ).wait_recv()

    def pass_on(self, k):
        self.arrived(self.peer(k))
        self.relay_copy(k).start()

    def other(self, k):
        return self.peer(k) + 1 - 2 * self.core

    def finish(self):
        for copy in self.copies():
            copy.wait_send()
        for k in range(1, self.n // 2):
            self.relay_copy(k).wait_send()


def kernel(
    n,
    m,
    turn,
    pos_hbm,
    q_hbm,
    kv_hbm,
    g_hbm,
    w_hbm,
    dq_ref,
    dw_ref,
    pos_ref,
    q_ref,
    kv_ref,
    g_v,
    gt_v,
    w_v,
    kv_all,
    part,
    part_all,
    attn_own,
    attn_all,
    g_all,
    scores,
    local_sem,
    kv_send,
    kv_relay,
    kv_recv,
    at_send,
    at_relay,
    at_recv,
    g_send,
    g_recv,
    p_send,
    p_recv,
):
    me = lax.axis_index("seq")
    hme = lax.axis_index("head")
    tok = q_ref.shape[0]
    heads = q_ref.shape[1] // HD
    rows = g_all.shape[1]
    dz = w_v.shape[0]
    scale = HD ** (-0.5)

    barrier = pltpu.get_barrier_semaphore()
    for k in range(1, n):
        pl.semaphore_signal(
            barrier, inc=1, device_id={"seq": lax.rem(me + k, n)}, device_id_type=MESH
        )
    for k in range(1, m):
        pl.semaphore_signal(
            barrier, inc=1, device_id={"head": lax.rem(hme + k, m)}, device_id_type=MESH
        )

    group = lax.div(hme * heads, GROUP)
    columns = pl.ds(pl.multiple_of(group * HD, HD), HD)
    own_kv = kv_ref.at[...]
    kv_copy = pltpu.make_async_copy(kv_hbm.at[:, :, columns], kv_ref, local_sem.at[0])
    g_copy = pltpu.make_async_copy(g_hbm, g_v, local_sem.at[1])
    w_copy = pltpu.make_async_copy(w_hbm, w_v, local_sem.at[2])
    q_copy = pltpu.make_async_copy(q_hbm, q_ref, local_sem.at[3])
    pos_copy = pltpu.make_async_copy(pos_hbm, pos_ref, local_sem.at[4])
    for copy in (kv_copy, g_copy, w_copy, q_copy, pos_copy):
        copy.start()
    kv_copy.wait()
    kv_all[me] = kv_ref[...]

    g_copy.wait()
    if turn:
        for j in range(n * rows // HD):
            gt_v[pl.ds(j * HD, HD), :] = g_v[:, pl.ds(j * HD, HD)].T

        def g_block(i):
            return gt_v.at[pl.ds(pl.multiple_of(i * rows, 16), rows)]

    else:

        def g_block(i):
            return g_v.at[i]

    pl.semaphore_wait(barrier, n + m - 2)
    kv = Gather(n, me, own_kv, kv_all, kv_send, kv_relay, kv_recv)
    kv.start()

    def g_send_copy(k):
        to = lax.rem(me + k, n)
        return remote(g_block(to), g_all.at[me], g_send.at[k], g_recv.at[me], "seq", to)

    for k in range(1, n):
        g_send_copy(k).start()

    w_copy.wait()

    def partial(j):
        wide = heads * HD
        total = jnp.zeros((tok, wide), jnp.float32)
        if turn:
            lhs = g_v[:, pl.ds(pl.multiple_of(hme * dz, HD), dz)]
            for h in range(heads):
                piece = jnp.dot(
                    lhs, w_v[:, j * heads + h, :], preferred_element_type=jnp.float32
                )
                yield piece
        else:
            blocks = dz // rows
            for h in range(heads):
                total = jnp.zeros((tok, HD), jnp.float32)
                for b in range(blocks):
                    total = total + lax.dot_general(
                        g_v[hme * blocks + b],
                        w_v[pl.ds(b * rows, rows), j * heads + h, :],
                        (((0,), (0,)), ((), ())),
                        preferred_element_type=jnp.float32,
                    )
                yield total

    for j in range(m):
        for h, piece in enumerate(partial(j)):
            part[j, :, pl.ds(h * HD, HD)] = piece.astype(jnp.bfloat16)

    def p_copy(k):
        to = lax.rem(hme + k, m)
        return remote(part.at[to], part_all.at[hme], p_send.at[k], p_recv.at[hme], "head", to)

    for k in range(1, m):
        p_copy(k).start()

    for k in range(1, n // 2):
        kv.pass_on(k)
    for k in range(n // 2):
        kv.arrived(kv.other(k))

    q_copy.wait()
    pos_copy.wait()
    query = jnp.concatenate([q_ref[:, pl.ds(h * HD, HD)] for h in range(heads)], axis=0)
    total_rows = heads * tok
    row = lax.broadcasted_iota(jnp.int32, (tok, 1), 0)
    lane = lax.broadcasted_iota(jnp.int32, (1, tok), 1)

    def run_positions(block, index):
        value = pos_ref[block * tok] + index
        for r in range(1, tok // RUN):
            start = pos_ref[block * tok + r * RUN] + index - r * RUN
            value = jnp.where(index >= r * RUN, start, value)
        return value

    own_pos = run_positions(me, row)
    query_pos = jnp.concatenate([own_pos] * heads, axis=0)
    step_blocks = min(n, 8)
    span = step_blocks * tok

    def keys(c, which):
        return kv_all[pl.ds(c * step_blocks, step_blocks), which].reshape(span, HD)

    def loop(body, init):
        if n == step_blocks:
            return body(0, init)
        return lax.fori_loop(0, n // step_blocks, body, init)

    def at(c):
        return pl.ds(c * span if isinstance(c, int) else pl.multiple_of(c * span, span), span)

    def score_step(c, top):
        value = lax.dot_general(
            query, keys(c, 0), (((1,), (1,)), ((), ())), preferred_element_type=jnp.float32
        )
        key_pos = jnp.concatenate(
            [run_positions(c * step_blocks + b, lane) for b in range(step_blocks)], axis=1
        )
        value = jnp.where(key_pos <= query_pos, value * scale, BIG_NEGATIVE)
        scores[:, at(c)] = value
        return jnp.maximum(top, jnp.max(value, axis=1, keepdims=True))

    top = loop(score_step, jnp.full((total_rows, 1), BIG_NEGATIVE, jnp.float32))

    def norm_step(c, norm):
        weights = jnp.exp(scores[:, at(c)] - top)
        scores[:, at(c)] = weights
        return norm + jnp.sum(weights, axis=1, keepdims=True)

    inverse = 1.0 / loop(norm_step, jnp.zeros((total_rows, 1), jnp.float32))

    def out_step(c, out):
        probs = scores[:, at(c)] * inverse
        scores[:, at(c)] = probs
        return out + jnp.dot(
            probs.astype(jnp.bfloat16), keys(c, 1), preferred_element_type=jnp.float32
        )

    attn = loop(out_step, jnp.zeros((total_rows, HD), jnp.float32))
    for h in range(heads):
        attn_own[:, pl.ds(h * HD, HD)] = attn[h * tok : (h + 1) * tok].astype(jnp.bfloat16)
    at_gather = Gather(n, me, attn_own, attn_all, at_send, at_relay, at_recv)
    at_gather.start()

    grad = part[hme].astype(jnp.float32)
    for k in range(1, m):
        src = lax.rem(hme + k, m)
        remote(
            part.at[0], part_all.at[src], p_send.at[k], p_recv.at[src], "head", src
        ).wait_recv()
        grad = grad + part_all[src].astype(jnp.float32)
    grad = jnp.concatenate(
        [grad[:, h * HD : (h + 1) * HD] for h in range(heads)], axis=0
    ).astype(jnp.bfloat16)
    delta = jnp.sum(grad.astype(jnp.float32) * attn, axis=1, keepdims=True)

    def grad_step(c, total):
        dprob = lax.dot_general(
            grad, keys(c, 1), (((1,), (1,)), ((), ())), preferred_element_type=jnp.float32
        )
        dscore = (scores[:, at(c)] * (dprob - delta)).astype(jnp.bfloat16)
        return total + jnp.dot(dscore, keys(c, 0), preferred_element_type=jnp.float32)

    d_rows = loop(grad_step, jnp.zeros((total_rows, HD), jnp.float32)) * scale
    for h in range(heads):
        dq_ref[:, pl.ds(h * HD, HD)] = d_rows[h * tok : (h + 1) * tok].astype(jnp.bfloat16)

    total = jnp.dot(g_block(me)[...], attn_own[...], preferred_element_type=jnp.float32)

    def g_arrived(src):
        remote(
            g_block(me), g_all.at[src], g_send.at[1], g_recv.at[src], "seq", src
        ).wait_recv()

    for k in range(1, n // 2):
        at_gather.pass_on(k)
    order = [at_gather.other(0)]
    for k in range(1, n // 2):
        order += [at_gather.peer(k), at_gather.other(k)]
    for index, src in enumerate(order):
        if index % 2 == 0:
            at_gather.arrived(src)
        g_arrived(src)
        total = total + jnp.dot(g_all[src], attn_all[src], preferred_element_type=jnp.float32)
    for h in range(heads):
        dw_ref[h] = total[:, h * HD : (h + 1) * HD]

    kv.finish()
    at_gather.finish()
    for k in range(1, n):
        g_send_copy(k).wait_send()
    for k in range(1, m):
        p_copy(k).wait_send()


def place(dq_in, dw_in, dq_ref, dw_ref):
    dq_ref[...] = dq_in[...]
    for h in range(dw_in.shape[0]):
        dw_ref[:, h, :] = dw_in[h]


def body(n, m, queries, keys_values, out_weight, out_grad, positions):
    tok, width = queries.shape
    heads = width // HD
    dz, all_heads, _ = out_weight.shape
    features = out_grad.shape[1]
    rows = features // n
    turn = rows % 16 == 0 and dz % HD == 0 and features % HD == 0
    bf16, f32 = jnp.bfloat16, jnp.float32
    if not turn:
        out_grad = out_grad.T.reshape(n, rows, tok)
    vmem = pl.BlockSpec(memory_space=pltpu.VMEM)
    anywhere = pl.BlockSpec(memory_space=pltpu.HBM)
    dma = pltpu.SemaphoreType.DMA
    buffers = [
        pltpu.VMEM((tok, width), bf16),
        pltpu.VMEM((2, tok, HD), bf16),
        pltpu.VMEM(out_grad.shape, bf16),
        pltpu.VMEM((features, tok) if turn else (16, HD), bf16),
        pltpu.VMEM(out_weight.shape, bf16),
        pltpu.VMEM((n, 2, tok, HD), bf16),
        pltpu.VMEM((m, tok, width), bf16),
        pltpu.VMEM((m, tok, width), bf16),
        pltpu.VMEM((tok, width), bf16),
        pltpu.VMEM((n, tok, width), bf16),
        pltpu.VMEM((n, rows, tok), bf16),
        pltpu.VMEM((heads * tok, n * tok), f32),
    ]
    results = 2 * tok * width + 4 * rows * width
    d_query, d_weight = pl.pallas_call(
        functools.partial(kernel, n, m, turn),
        out_shape=(
            jax.ShapeDtypeStruct((tok, width), bf16),
            jax.ShapeDtypeStruct((heads, rows, HD), f32),
        ),
        in_specs=[anywhere] * 5,
        out_specs=(vmem, vmem),
        scratch_shapes=[
            pltpu.SMEM(positions.shape, jnp.int32),
            *buffers,
            dma((5,)),
            dma((n,)),
            dma((n,)),
            dma((n,)),
            dma((n,)),
            dma((n,)),
            dma((n,)),
            dma((n,)),
            dma((n,)),
            dma((m,)),
            dma((m,)),
        ],
        compiler_params=pltpu.CompilerParams(
            collective_id=0, has_side_effects=True, vmem_limit_bytes=VMEM_LIMIT - results - (24 << 10)
        ),
    )(positions, queries, keys_values, out_grad, out_weight)
    return pl.pallas_call(
        place,
        out_shape=(
            jax.ShapeDtypeStruct((tok, width), bf16),
            jax.ShapeDtypeStruct((rows, heads, HD), f32),
        ),
        in_specs=[vmem, vmem],
        out_specs=(vmem, vmem),
        compiler_params=pltpu.CompilerParams(vmem_limit_bytes=4 << 20),
        cost_estimate=pl.CostEstimate(flops=1 << 20, bytes_accessed=1 << 20, transcendentals=0),
    )(d_query, d_weight)


def solution(mesh):
    n, m = mesh.shape["seq"], mesh.shape["head"]
    return jax.shard_map(
        functools.partial(body, n, m),
        mesh=mesh,
        in_specs=(
            P("seq", "head"),
            P(None, "seq", None),
            P("head", None, None),
            P("seq", None),
            P(),
        ),
        out_specs=(P("seq", "head"), P("seq", "head", None)),
        check_vma=False,
    )
```
